32 devices in a mesh: grp: 2 (over core), tab: 16 (over z, y, x).
Axes of the slice: x: 2, y: 2, z: 4, core: 2. Of those that a mesh axis runs over, the one named last changes fastest.
Arguments:
- sample_ids: int32 [4, 1024, 1024], P(None, ('grp', 'tab')), may hold values from 0 to 1535
- id_weights: bfloat16 [4, 1024, 1024], P(None, ('grp', 'tab')), may hold values from 0.25 to 2
- dense_features: bfloat16 [4, 1024, 128], P(None, ('grp', 'tab')), may hold values from -6 to 6
- click_labels: int32 [4, 1024], P(None, ('grp', 'tab')), may hold values 0 or 1
- table_shards: bfloat16 [128, 1536, 128], P('tab'), may hold values from -1.1953125 to 1.1953125
- slot_table: int32 [128], replicated, may hold values from 0 to 127, each once
- top_weight: bfloat16 [128, 1024], replicated, may hold values from -0.5 to 0.5
- top_bias: float32 [1024], replicated, may hold values from -3 to 3
- out_weight: bfloat16 [1024], replicated, may hold values from -0.1875 to 0.1875
Outputs:
- logits: float32 [4, 1024], P(None, ('grp', 'tab'))
- grad_top: float32 [128, 1024], replicated
- grad_bias: float32 [1024], replicated
The draws below stay inside these ranges and needn't reach their ends.
Inputs may be any that keep to these rules, and one draw needn't show every extreme that they name: `slot_table`: a permutation: each table stands in exactly one slot.
All inputs are finite; a program needn't handle non-finite values. No bound on the sum of `click_labels` on one device may be relied on, other than what follows from the above.
Results may differ from the reference program's by a relative error of at most 0.0056.
Values may be sent and summed in bfloat16 or wider, within the bound.
No kernel may reach another device: no remote copies, remote signals or barrier semaphores. Data moves between devices by JAX's collectives and lax.ppermute only.
A program may use at most 128 MiB of HBM per device.

```python
import math
import jax
import jax.numpy as jnp
import numpy as np
from jax import lax

DIM = 128
VOCAB = 1536
HIDDEN_SIZE = 1024
HOTS = 8
MB = 4
TABLES = 128
BATCH = 1024


def place_ends(entries, key, smallest, largest):
    dims = entries.shape
    spot = [jax.random.randint(jax.random.fold_in(key, axis), (), 0, dims[axis]) for axis in range(len(dims))]
    entries = entries.at[tuple(spot)].set(smallest)
    longest = dims.index(max(dims))
    spot[longest] = (spot[longest] + 1) % dims[longest]
    return entries.at[tuple(spot)].set(largest)


def shard_levels(stream_key, dims, cuts, low, high):
    level, own = 1.0, jax.random.fold_in(stream_key, 6)
    for dim, blocks in cuts:
        steps = jnp.exp(jax.random.uniform(jax.random.fold_in(own, dim), (blocks,), jnp.float32, low / len(cuts), high / len(cuts)))
        level = level * jnp.repeat(steps, dims[dim] // blocks).reshape([-1 if axis == dim else 1 for axis in range(len(dims))])
    return level


def cumulative_ranks(count, lean):
    weights = [(1 << 20) // math.isqrt(standing ** lean) + 1 for standing in range(1, count + 1)]
    spread = 1 + sum(weights) // (1 << 30)
    return np.cumsum(np.array([max(1, weight // spread) for weight in weights]))


def skewed_ids(own_key, shape, number_of, skew):
    table = cumulative_ranks(number_of, skew)
    pick = jax.random.randint(jax.random.fold_in(own_key, 1), shape, 0, int(table[number_of - 1]))
    standing = jnp.searchsorted(jnp.asarray(table, jnp.int32), pick, side="right")
    return jax.random.permutation(jax.random.fold_in(own_key, 2), number_of)[standing].astype(jnp.int32)


def bell_draw(own_key, dims, width, bound, shards=(), kind=jnp.bfloat16):
    drawn = jax.random.normal(own_key, dims, jnp.float32) * width
    if len(shards) > 0:
        drawn = shard_levels(own_key, dims, shards, -0.22, 0.18) * drawn
    return jnp.clip(drawn, min=-bound, max=bound).astype(kind)


def setup_inputs(seed: int = 0) -> dict:
    key_list = jax.random.split(jax.random.key(seed), 10)
    return {
        "sample_ids": place_ends(skewed_ids(key_list[0], (MB, BATCH, TABLES * HOTS), VOCAB, 2), jax.random.fold_in(key_list[0], 3), 0, VOCAB - 1).astype(jnp.int32),
        "id_weights": jnp.clip(0.25 + 1.75 * jax.random.uniform(key_list[1], (MB, BATCH, TABLES * HOTS), jnp.float32) ** shard_levels(key_list[1], (MB, BATCH, TABLES * HOTS), ((1, 32),), -0.2, 0.2), 0.25, 2.0).astype(jnp.bfloat16),
        "dense_features": bell_draw(key_list[2], (MB, BATCH, DIM), 1.0, 6.0, ((1, 32),)),
        "click_labels": place_ends((jax.random.randint(key_list[3], (MB, BATCH), 0, 2) < 1).astype(jnp.int32), jax.random.fold_in(key_list[3], 1), 0, 1),
        "table_shards": bell_draw(key_list[4], (TABLES, VOCAB, DIM), 0.2, 1.1953125, ((0, 16),)),
        "slot_table": jax.random.permutation(key_list[5], TABLES).astype(jnp.int32),
        "top_weight": bell_draw(key_list[6], (TABLES, HIDDEN_SIZE), TABLES ** -0.5, 0.5),
        "top_bias": bell_draw(key_list[7], (HIDDEN_SIZE,), 0.5, 3.0, (), jnp.float32),
        "out_weight": bell_draw(key_list[8], (HIDDEN_SIZE,), HIDDEN_SIZE ** -0.5, 0.1875),
    }


loss_scale = 32768.0

def reference(sample_ids, id_weights, dense_features, click_labels, table_shards, slot_table, top_weight, top_bias, out_weight):
    count = MB * BATCH
    ids_all = sample_ids.reshape(count, TABLES, HOTS)
    weights_all = id_weights.reshape(count, TABLES, HOTS).astype(jnp.float32)
    features = dense_features.reshape(count, DIM).astype(jnp.float32)
    earlier = jnp.arange(HOTS)[None, :] < jnp.arange(HOTS)[:, None]
    scale = 1.0 / jnp.sqrt(jnp.float32(DIM))

    def slot_scores(slot):
        table = slot_table[slot]
        slot_ids = lax.dynamic_index_in_dim(ids_all, table, axis=1, keepdims=False)
        slot_weights = lax.dynamic_index_in_dim(weights_all, table, axis=1, keepdims=False)
        same = slot_ids[:, :, None] == slot_ids[:, None, :]
        summed = lax.optimization_barrier(jnp.sum(jnp.where(same, slot_weights[:, None, :], jnp.float32(0.0)), axis=2))
        first = jnp.logical_not(jnp.any(same & earlier[None], axis=2))
        rounded = lax.optimization_barrier(summed.astype(jnp.bfloat16)).astype(jnp.float32)
        merged = jnp.where(first, rounded, jnp.float32(0.0))
        shard = lax.dynamic_index_in_dim(table_shards, slot, axis=0, keepdims=False)
        rows = shard[slot_ids].astype(jnp.float32)
        pooled = jnp.einsum('nh,nhe->ne', merged, rows).astype(jnp.bfloat16)
        pooled_wide = lax.optimization_barrier(pooled).astype(jnp.float32)
        return (lax.optimization_barrier(jnp.sum(pooled_wide * features, axis=1)) * scale).astype(jnp.bfloat16)
    scores = lax.map(slot_scores, jnp.arange(TABLES, dtype=jnp.int32)).T
    slot_weight = top_weight[slot_table]
    pre = jnp.dot(scores, slot_weight, preferred_element_type=jnp.float32) + top_bias
    gate = jax.nn.sigmoid(pre)
    hidden = (pre * gate).astype(jnp.bfloat16)
    logit_all = jnp.dot(hidden, out_weight, preferred_element_type=jnp.float32)
    labels = click_labels.reshape(count).astype(jnp.float32)
    delta = (jax.nn.sigmoid(logit_all) - labels) * (loss_scale / count)
    slope = gate * (1.0 + pre * (1.0 - gate))
    hidden_grad = (delta[:, None] * out_weight.astype(jnp.float32)[None, :] * slope).astype(jnp.bfloat16)
    hidden_grad = lax.optimization_barrier(hidden_grad)
    grad_slot = jnp.dot(scores.T, hidden_grad, preferred_element_type=jnp.float32)
    grad_bias = lax.optimization_barrier(jnp.sum(hidden_grad.astype(jnp.float32), axis=0))
    grad_top = jnp.zeros_like(grad_slot).at[slot_table].set(grad_slot)
    return (logit_all.reshape(MB, BATCH), grad_top, grad_bias)
```

```python
import functools
import math

import jax
import jax.numpy as jnp
from jax import lax
from jax.experimental import pallas as pl
from jax.experimental.pallas import tpu as pltpu
from jax.sharding import PartitionSpec as P

HOTS = 8
LOSS_SCALE = 32768.0
LANES = 128
SUB = 16
NT = (((1,), (1,)), ((), ()))


def pack_kernel(ids_ref, weights_ref, features_ref, labels_ref, rows_ref, out_ref, *, high, slots):
    members = out_ref.shape[0]
    columns = ids_ref.shape[1]
    block = slots * HOTS
    ids = ids_ref[...].astype(jnp.float32)
    tile = jnp.floor((ids + 0.5) * (1.0 / (SUB * high)))
    rest = ids - tile * (SUB * high)
    hi = jnp.floor((rest + 0.5) * (1.0 / SUB))
    code = rest - hi * SUB + tile * SUB + 128.0
    for bit in (1, 2, 4, 8):
        half = jnp.floor(hi * 0.5)
        code = jnp.where(hi - 2.0 * half > 0.5, code * float(2**bit), code)
        hi = half
    code = code.astype(jnp.bfloat16)
    weights = weights_ref[...]
    eye_r = lax.broadcasted_iota(jnp.int32, (LANES, LANES), 0)
    eye_c = lax.broadcasted_iota(jnp.int32, (LANES, LANES), 1)
    eye = jnp.where(eye_r == eye_c, 1.0, 0.0).astype(jnp.bfloat16)
    turned = lax.dot_general(eye, features_ref[...], NT, preferred_element_type=jnp.float32)
    turned = turned.astype(jnp.bfloat16)
    labels = labels_ref[...].astype(jnp.bfloat16)
    column = lax.broadcasted_iota(jnp.int32, (block, columns), 1)
    for member in range(members):
        rows = rows_ref[member * block : (member + 1) * block, :]
        pick = jnp.where(rows == column, 1.0, 0.0).astype(jnp.bfloat16)
        out_ref[member, 0:block, :] = lax.dot_general(
            pick, code, NT, preferred_element_type=jnp.float32
        ).astype(jnp.bfloat16)
        out_ref[member, block : 2 * block, :] = lax.dot_general(
            pick, weights, NT, preferred_element_type=jnp.float32
        ).astype(jnp.bfloat16)
        out_ref[member, 2 * block : 2 * block + LANES, :] = turned
        out_ref[member, 2 * block + LANES :, :] = labels


def pool_kernel(recv_ref, table_ref, out_ref, hi_ref, lo_ref, w_ref, part_ref, count_ref, acc_ref, *, high, slots, scale):
    slot = pl.program_id(0)
    members = recv_ref.shape[0]
    block = slots * HOTS
    tiles = 128 // SUB

    @pl.when(slot == 0)
    def _():
        def decode(src, carry):
            value = recv_ref[src, 0:block, :].astype(jnp.float32)
            hi = jnp.zeros_like(value)
            for bit in (8, 4, 2, 1):
                big = value >= 128.0 * 2.0**bit
                value = jnp.where(big, value * 2.0**-bit, value)
                hi = jnp.where(big, hi + float(bit), hi)
            hi_ref[src] = hi
            lo_ref[src] = value - 128.0
            w_ref[src] = recv_ref[src, block : 2 * block, :].astype(jnp.float32)
            return carry

        lax.fori_loop(0, members, decode, 0)

    iota = lax.broadcasted_iota(jnp.int32, (SUB, LANES), 0).astype(jnp.float32).astype(jnp.bfloat16)
    zero = jnp.zeros((SUB, LANES), jnp.bfloat16)
    first = pl.multiple_of(slot * HOTS, HOTS)

    def spread(row):
        return jnp.broadcast_to(row, (SUB, LANES)).astype(jnp.bfloat16)

    def pair(index, carry):
        for side in range(2):
            src = index * 2 + side
            hi8 = hi_ref[src, pl.ds(first, HOTS), :]
            lo8 = lo_ref[src, pl.ds(first, HOTS), :]
            w8 = w_ref[src, pl.ds(first, HOTS), :]
            lows = []
            for hot in range(HOTS):
                hi_b = spread(hi8[hot : hot + 1])
                w_b = spread(w8[hot : hot + 1])
                lows.append(spread(lo8[hot : hot + 1]))
                for k in range(high):
                    part_ref[side, hot * high + k] = jnp.where(hi_b == jnp.bfloat16(k), w_b, zero)
            for tile in range(tiles):
                here = iota + jnp.bfloat16(tile * SUB)
                masks = [low == here for low in lows]
                for k in range(high):
                    total = jnp.where(masks[0], part_ref[side, k], zero)
                    for hot in range(1, HOTS):
                        total = total + jnp.where(masks[hot], part_ref[side, hot * high + k], zero)
                    base = (tile * high + k) * SUB
                    count_ref[base : base + SUB, side * LANES : (side + 1) * LANES] = total
        pooled = jnp.dot(table_ref[0], count_ref[...], preferred_element_type=jnp.float32)
        pooled = pooled.astype(jnp.bfloat16).astype(jnp.float32)
        for side in range(2):
            src = index * 2 + side
            turned = recv_ref[src, 2 * block : 2 * block + LANES, :].astype(jnp.float32)
            dots = jnp.sum(pooled[:, side * LANES : (side + 1) * LANES] * turned, axis=0, keepdims=True)
            acc_ref[src, pl.ds(slot, 1), :] = dots * scale
        return carry

    lax.fori_loop(0, members // 2, pair, 0)

    @pl.when(slot == slots - 1)
    def _():
        for src in range(members):
            out_ref[:, src * LANES : (src + 1) * LANES] = acc_ref[src].astype(jnp.bfloat16)


def top_kernel(scores_ref, labels_ref, place_ref, weight_ref, bias_ref, wide_ref, narrow_ref, logits_ref, grad_ref, slope_ref, bias_b, wide_b, *, factor):
    hidden_size = weight_ref.shape[0]
    chunk = 256
    samples = 2 * LANES

    @pl.when(pl.program_id(0) == 0)
    def _():
        grad_ref[...] = jnp.zeros_like(grad_ref)
        bias_b[...] = jnp.broadcast_to(bias_ref[...], bias_b.shape)
        wide_b[...] = jnp.broadcast_to(wide_ref[...], wide_b.shape)

    scores = jnp.dot(place_ref[...], scores_ref[...], preferred_element_type=jnp.float32)
    scores = scores.astype(jnp.bfloat16)
    logits = jnp.zeros((8, samples), jnp.float32)
    for start in range(0, hidden_size, chunk):
        span = slice(start, start + chunk)
        bias = jnp.concatenate([bias_b[span, :]] * 2, axis=1)
        wide = jnp.concatenate([wide_b[span, :]] * 2, axis=1)
        pre = jnp.dot(weight_ref[span, :], scores, preferred_element_type=jnp.float32) + bias
        gate = 0.5 + 0.5 * jnp.tanh(0.5 * pre)
        hidden = pre * gate
        logits = logits + jnp.dot(
            narrow_ref[:, span], hidden.astype(jnp.bfloat16), preferred_element_type=jnp.float32
        )
        slope_ref[span, :] = wide * (gate + hidden * (1.0 - gate))
    logits_ref[...] = logits
    labels = jnp.concatenate([labels_ref[0, 0:1, :], labels_ref[1, 0:1, :]], axis=1)
    delta = (0.5 + 0.5 * jnp.tanh(0.5 * logits[0:1, :]) - labels.astype(jnp.float32)) * factor
    ones = jnp.ones((SUB, samples), jnp.bfloat16)
    left = jnp.concatenate([scores, ones], axis=0)
    for start in range(0, hidden_size, chunk):
        span = slice(start, start + chunk)
        hidden_grad = (slope_ref[span, :] * delta).astype(jnp.bfloat16)
        grad_ref[:, span] += lax.dot_general(left, hidden_grad, NT, preferred_element_type=jnp.float32)


def per_device(
    sample_ids,
    id_weights,
    dense_features,
    click_labels,
    table_shards,
    slot_table,
    top_weight,
    top_bias,
    out_weight,
):
    micro, local_batch, columns = sample_ids.shape
    tables = slot_table.shape[0]
    slots, vocab, width = table_shards.shape
    hidden_size = top_weight.shape[1]
    members = lax.axis_size("tab")
    groups = lax.axis_size("grp")
    local = micro * local_batch
    high = vocab // 128
    assert local == LANES and width == LANES and vocab % 128 == 0 and high <= 16 and members % 2 == 0
    block = slots * HOTS
    height = 2 * block + LANES + SUB
    scale = 1.0 / math.sqrt(width)

    rows = (slot_table[:, None] * HOTS + jnp.arange(HOTS, dtype=jnp.int32)[None, :]).reshape(columns, 1)
    labels = jnp.broadcast_to(click_labels.reshape(1, local), (SUB, local)).astype(jnp.float32)
    packed = pl.pallas_call(
        functools.partial(pack_kernel, high=high, slots=slots),
        out_shape=jax.ShapeDtypeStruct((members, height, LANES), jnp.bfloat16),
        name="pack",
    )(
        sample_ids.reshape(local, columns),
        id_weights.reshape(local, columns),
        dense_features.reshape(local, width),
        labels,
        rows,
    )
    received = lax.all_to_all(packed, "tab", split_axis=0, concat_axis=0, tiled=True)
    turned_tables = jnp.swapaxes(table_shards, 1, 2)
    samples = members * LANES
    scores = pl.pallas_call(
        functools.partial(pool_kernel, high=high, slots=slots, scale=scale),
        grid=(slots,),
        in_specs=[
            pl.BlockSpec((members, height, LANES), lambda s: (0, 0, 0)),
            pl.BlockSpec((1, width, vocab), lambda s: (s, 0, 0)),
        ],
        out_specs=pl.BlockSpec((slots, samples), lambda s: (0, 0)),
        out_shape=jax.ShapeDtypeStruct((slots, samples), jnp.bfloat16),
        scratch_shapes=[
            pltpu.VMEM((members, block, LANES), jnp.float32),
            pltpu.VMEM((members, block, LANES), jnp.float32),
            pltpu.VMEM((members, block, LANES), jnp.float32),
            pltpu.VMEM((2, HOTS * high, SUB, LANES), jnp.bfloat16),
            pltpu.VMEM((vocab, 2 * LANES), jnp.bfloat16),
            pltpu.VMEM((members, slots, LANES), jnp.float32),
        ],
        name="pool",
    )(received, turned_tables)
    gathered = lax.all_gather(scores, "tab", axis=0, tiled=True)
    place = (jnp.arange(tables, dtype=jnp.int32)[:, None] == slot_table[None, :]).astype(jnp.bfloat16)
    label_block = (2 * block + LANES) // SUB
    logits, grad = pl.pallas_call(
        functools.partial(top_kernel, factor=LOSS_SCALE / (local * members * groups)),
        grid=(members // 2,),
        in_specs=[
            pl.BlockSpec((tables, 2 * LANES), lambda j: (0, j)),
            pl.BlockSpec((2, SUB, LANES), lambda j: (j, label_block, 0)),
            pl.BlockSpec((tables, tables), lambda j: (0, 0)),
            pl.BlockSpec((hidden_size, tables), lambda j: (0, 0)),
            pl.BlockSpec((hidden_size, 1), lambda j: (0, 0)),
            pl.BlockSpec((hidden_size, 1), lambda j: (0, 0)),
            pl.BlockSpec((8, hidden_size), lambda j: (0, 0)),
        ],
        out_specs=[
            pl.BlockSpec((8, 2 * LANES), lambda j: (0, j)),
            pl.BlockSpec((tables + SUB, hidden_size), lambda j: (0, 0)),
        ],
        out_shape=[
            jax.ShapeDtypeStruct((8, samples), jnp.float32),
            jax.ShapeDtypeStruct((tables + SUB, hidden_size), jnp.float32),
        ],
        scratch_shapes=[
            pltpu.VMEM((hidden_size, 2 * LANES), jnp.float32),
            pltpu.VMEM((hidden_size, LANES), jnp.float32),
            pltpu.VMEM((hidden_size, LANES), jnp.float32),
        ],
        name="top",
    )(
        gathered,
        received,
        place,
        top_weight.T,
        top_bias.reshape(hidden_size, 1),
        out_weight.astype(jnp.float32).reshape(hidden_size, 1),
        jnp.broadcast_to(out_weight[None, :], (8, hidden_size)),
    )
    if groups == 2:
        grad = grad + lax.ppermute(grad, "grp", [(0, 1), (1, 0)])
    else:
        grad = lax.psum(grad, "grp")
    own = lax.dynamic_slice(logits, (0, lax.axis_index("tab") * LANES), (1, LANES))
    return own.reshape(micro, local_batch), grad[:tables], grad[tables]


def solution(mesh):
    return jax.shard_map(
        per_device,
        mesh=mesh,
        in_specs=(
            P(None, ("grp", "tab"), None),
            P(None, ("grp", "tab"), None),
            P(None, ("grp", "tab"), None),
            P(None, ("grp", "tab")),
            P("tab", None, None),
            P(),
            P(),
            P(),
            P(),
        ),
        out_specs=(P(None, ("grp", "tab")), P(), P()),
        check_vma=False,
    )
```

```python
import functools
import math

import jax
import jax.numpy as jnp
from jax import lax
from jax.experimental import pallas as pl
from jax.experimental.pallas import tpu as pltpu
from jax.sharding import PartitionSpec as P

HOTS = 8
LOSS_SCALE = 32768.0
LANES = 128
SUB = 16
NT = (((1,), (1,)), ((), ()))


def pack_kernel(ids_ref, weights_ref, features_ref, labels_ref, rows_ref, out_ref, *, high, slots):
    members = out_ref.shape[0]
    columns = ids_ref.shape[1]
    block = slots * HOTS
    ids = ids_ref[...].astype(jnp.float32)
    tile = jnp.floor((ids + 0.5) * (1.0 / (SUB * high)))
    rest = ids - tile * (SUB * high)
    hi = jnp.floor((rest + 0.5) * (1.0 / SUB))
    code = rest - hi * SUB + tile * SUB + 128.0
    for bit in (1, 2, 4, 8):
        half = jnp.floor(hi * 0.5)
        code = jnp.where(hi - 2.0 * half > 0.5, code * float(2**bit), code)
        hi = half
    code = code.astype(jnp.bfloat16)
    weights = weights_ref[...]
    eye_r = lax.broadcasted_iota(jnp.int32, (LANES, LANES), 0)
    eye_c = lax.broadcasted_iota(jnp.int32, (LANES, LANES), 1)
    eye = jnp.where(eye_r == eye_c, 1.0, 0.0).astype(jnp.bfloat16)
    turned = lax.dot_general(eye, features_ref[...], NT, preferred_element_type=jnp.float32)
    turned = turned.astype(jnp.bfloat16)
    labels = labels_ref[...].astype(jnp.bfloat16)
    column = lax.broadcasted_iota(jnp.int32, (block, columns), 1)
    for member in range(members):
        rows = rows_ref[member * block : (member + 1) * block, :]
        pick = jnp.where(rows == column, 1.0, 0.0).astype(jnp.bfloat16)
        out_ref[member, 0:block, :] = lax.dot_general(
            pick, code, NT, preferred_element_type=jnp.float32
        ).astype(jnp.bfloat16)
        out_ref[member, block : 2 * block, :] = lax.dot_general(
            pick, weights, NT, preferred_element_type=jnp.float32
        ).astype(jnp.bfloat16)
        out_ref[member, 2 * block : 2 * block + LANES, :] = turned
        out_ref[member, 2 * block + LANES :, :] = labels


def pool_kernel(recv_ref, table_ref, out_ref, hi_ref, lo_ref, w_ref, part_ref, low_ref, even_ref, odd_ref, sum_ref, acc_ref, *, high, slots, scale):
    slot = pl.program_id(0)
    members = recv_ref.shape[0]
    block = slots * HOTS
    pairs = members // 2
    steps = even_ref.shape[0]

    @pl.when(slot == 0)
    def _():
        def decode(src, carry):
            value = recv_ref[src, 0:block, :].astype(jnp.float32)
            hi = jnp.zeros_like(value)
            for bit in (8, 4, 2, 1):
                big = value >= 128.0 * 2.0**bit
                value = jnp.where(big, value * 2.0**-bit, value)
                hi = jnp.where(big, hi + float(bit), hi)
            hi_ref[src] = hi
            lo_ref[src] = value - 128.0
            w_ref[src] = recv_ref[src, block : 2 * block, :].astype(jnp.float32)
            return carry

        lax.fori_loop(0, members, decode, 0)

    iota = lax.broadcasted_iota(jnp.int32, (SUB, LANES), 0).astype(jnp.float32)
    zero = jnp.zeros((SUB, LANES), jnp.bfloat16)
    first = pl.multiple_of(slot * HOTS, HOTS)

    def spread(row):
        return jnp.broadcast_to(row, (SUB, LANES)).astype(jnp.bfloat16)

    def count(pair, new_ref, old_ref):
        for side in range(2):
            src = pair * 2 + side
            hi8 = hi_ref[src, pl.ds(first, HOTS), :]
            lo8 = lo_ref[src, pl.ds(first, HOTS), :]
            w8 = w_ref[src, pl.ds(first, HOTS), :]
            for hot in range(HOTS):
                hi_b = spread(hi8[hot : hot + 1])
                w_b = spread(w8[hot : hot + 1])
                low_ref[side, hot] = spread(lo8[hot : hot + 1])
                for k in range(high):
                    part_ref[side, hot * high + k] = jnp.where(hi_b == jnp.bfloat16(k), w_b, zero)
        if old_ref is not None:
            sum_ref[...] = jnp.zeros_like(sum_ref)

        def step(q, carry):
            if old_ref is not None:
                sum_ref[...] += jnp.dot(table_ref[0, q], old_ref[q], preferred_element_type=jnp.float32)
            start = (q * (2 * SUB)).astype(jnp.float32)
            here = [(iota + (start + t * SUB)).astype(jnp.bfloat16) for t in range(2)]
            for side in range(2):
                totals = [[None] * high for _ in range(2)]
                for hot in range(HOTS):
                    low = low_ref[side, hot]
                    masks = [low == here[t] for t in range(2)]
                    for k in range(high):
                        part = part_ref[side, hot * high + k]
                        for t in range(2):
                            addend = jnp.where(masks[t], part, zero)
                            totals[t][k] = addend if hot == 0 else totals[t][k] + addend
                for t in range(2):
                    for k in range(high):
                        base = (t * high + k) * SUB
                        new_ref[q, base : base + SUB, side * LANES : (side + 1) * LANES] = totals[t][k]
            return carry

        lax.fori_loop(0, steps, step, 0)

    def finish(pair):
        pooled = sum_ref[...].astype(jnp.bfloat16).astype(jnp.float32)
        for side in range(2):
            src = pair * 2 + side
            turned = recv_ref[src, 2 * block : 2 * block + LANES, :].astype(jnp.float32)
            dots = jnp.sum(pooled[:, side * LANES : (side + 1) * LANES] * turned, axis=0, keepdims=True)
            acc_ref[src, pl.ds(slot, 1), :] = dots * scale

    count(0, even_ref, None)

    def two(index, carry):
        count(2 * index + 1, odd_ref, even_ref)
        finish(2 * index)

        @pl.when(index < pairs // 2 - 1)
        def _():
            count(2 * index + 2, even_ref, odd_ref)
            finish(2 * index + 1)

        return carry

    lax.fori_loop(0, pairs // 2, two, 0)
    last = jnp.zeros(sum_ref.shape, jnp.float32)
    for q in range(steps):
        last = last + jnp.dot(table_ref[0, q], odd_ref[q], preferred_element_type=jnp.float32)
    sum_ref[...] = last
    finish(pairs - 1)

    @pl.when(slot == slots - 1)
    def _():
        for src in range(members):
            out_ref[:, src * LANES : (src + 1) * LANES] = acc_ref[src].astype(jnp.bfloat16)


def top_kernel(scores_ref, labels_ref, place_ref, weight_ref, bias_ref, wide_ref, narrow_ref, logits_ref, grad_ref, slope_ref, bias_b, wide_b, *, factor):
    hidden_size = weight_ref.shape[0]
    chunk = 256
    samples = 2 * LANES

    @pl.when(pl.program_id(0) == 0)
    def _():
        grad_ref[...] = jnp.zeros_like(grad_ref)
        bias_b[...] = jnp.broadcast_to(bias_ref[...], bias_b.shape)
        wide_b[...] = jnp.broadcast_to(wide_ref[...], wide_b.shape)

    scores = jnp.dot(place_ref[...], scores_ref[...], preferred_element_type=jnp.float32)
    scores = scores.astype(jnp.bfloat16)
    logits = jnp.zeros((8, samples), jnp.float32)
    for start in range(0, hidden_size, chunk):
        span = slice(start, start + chunk)
        bias = jnp.concatenate([bias_b[span, :]] * 2, axis=1)
        wide = jnp.concatenate([wide_b[span, :]] * 2, axis=1)
        pre = jnp.dot(weight_ref[span, :], scores, preferred_element_type=jnp.float32) + bias
        gate = 0.5 + 0.5 * jnp.tanh(0.5 * pre)
        hidden = pre * gate
        logits = logits + jnp.dot(
            narrow_ref[:, span], hidden.astype(jnp.bfloat16), preferred_element_type=jnp.float32
        )
        slope_ref[span, :] = wide * (gate + hidden * (1.0 - gate))
    logits_ref[...] = logits
    labels = jnp.concatenate([labels_ref[0, 0:1, :], labels_ref[1, 0:1, :]], axis=1)
    delta = (0.5 + 0.5 * jnp.tanh(0.5 * logits[0:1, :]) - labels.astype(jnp.float32)) * factor
    ones = jnp.ones((SUB, samples), jnp.bfloat16)
    left = jnp.concatenate([scores, ones], axis=0)
    for start in range(0, hidden_size, chunk):
        span = slice(start, start + chunk)
        hidden_grad = (slope_ref[span, :] * delta).astype(jnp.bfloat16)
        grad_ref[:, span] += lax.dot_general(left, hidden_grad, NT, preferred_element_type=jnp.float32)


def per_device(
    sample_ids,
    id_weights,
    dense_features,
    click_labels,
    table_shards,
    slot_table,
    top_weight,
    top_bias,
    out_weight,
):
    micro, local_batch, columns = sample_ids.shape
    tables = slot_table.shape[0]
    slots, vocab, width = table_shards.shape
    hidden_size = top_weight.shape[1]
    members = lax.axis_size("tab")
    groups = lax.axis_size("grp")
    local = micro * local_batch
    high = vocab // 128
    assert local == LANES and width == LANES and vocab % 128 == 0 and high <= 16 and members % 4 == 0
    block = slots * HOTS
    height = 2 * block + LANES + SUB
    scale = 1.0 / math.sqrt(width)

    rows = (slot_table[:, None] * HOTS + jnp.arange(HOTS, dtype=jnp.int32)[None, :]).reshape(columns, 1)
    labels = jnp.broadcast_to(click_labels.reshape(1, local), (SUB, local)).astype(jnp.float32)
    packed = pl.pallas_call(
        functools.partial(pack_kernel, high=high, slots=slots),
        out_shape=jax.ShapeDtypeStruct((members, height, LANES), jnp.bfloat16),
        name="pack",
    )(
        sample_ids.reshape(local, columns),
        id_weights.reshape(local, columns),
        dense_features.reshape(local, width),
        labels,
        rows,
    )
    received = lax.all_to_all(packed, "tab", split_axis=0, concat_axis=0, tiled=True)
    steps = 128 // (2 * SUB)
    turned_tables = jnp.swapaxes(table_shards.reshape(slots, steps, vocab // steps, width), 2, 3)
    samples = members * LANES
    scores = pl.pallas_call(
        functools.partial(pool_kernel, high=high, slots=slots, scale=scale),
        grid=(slots,),
        in_specs=[
            pl.BlockSpec((members, height, LANES), lambda s: (0, 0, 0)),
            pl.BlockSpec((1, steps, width, vocab // steps), lambda s: (s, 0, 0, 0)),
        ],
        out_specs=pl.BlockSpec((slots, samples), lambda s: (0, 0)),
        out_shape=jax.ShapeDtypeStruct((slots, samples), jnp.bfloat16),
        scratch_shapes=[
            pltpu.VMEM((members, block, LANES), jnp.float32),
            pltpu.VMEM((members, block, LANES), jnp.float32),
            pltpu.VMEM((members, block, LANES), jnp.float32),
            pltpu.VMEM((2, HOTS * high, SUB, LANES), jnp.bfloat16),
            pltpu.VMEM((2, HOTS, SUB, LANES), jnp.bfloat16),
            pltpu.VMEM((steps, vocab // steps, 2 * LANES), jnp.bfloat16),
            pltpu.VMEM((steps, vocab // steps, 2 * LANES), jnp.bfloat16),
            pltpu.VMEM((width, 2 * LANES), jnp.float32),
            pltpu.VMEM((members, slots, LANES), jnp.float32),
        ],
        name="pool",
    )(received, turned_tables)
    copies = jnp.broadcast_to(scores[None], (members, slots, samples))
    gathered = lax.all_to_all(copies, "tab", split_axis=0, concat_axis=0, tiled=True)
    gathered = gathered.reshape(tables, samples)
    place = (jnp.arange(tables, dtype=jnp.int32)[:, None] == slot_table[None, :]).astype(jnp.bfloat16)
    label_block = (2 * block + LANES) // SUB
    logits, grad = pl.pallas_call(
        functools.partial(top_kernel, factor=LOSS_SCALE / (local * members * groups)),
        grid=(members // 2,),
        in_specs=[
            pl.BlockSpec((tables, 2 * LANES), lambda j: (0, j)),
            pl.BlockSpec((2, SUB, LANES), lambda j: (j, label_block, 0)),
            pl.BlockSpec((tables, tables), lambda j: (0, 0)),
            pl.BlockSpec((hidden_size, tables), lambda j: (0, 0)),
            pl.BlockSpec((hidden_size, 1), lambda j: (0, 0)),
            pl.BlockSpec((hidden_size, 1), lambda j: (0, 0)),
            pl.BlockSpec((8, hidden_size), lambda j: (0, 0)),
        ],
        out_specs=[
            pl.BlockSpec((8, 2 * LANES), lambda j: (0, j)),
            pl.BlockSpec((tables + SUB, hidden_size), lambda j: (0, 0)),
        ],
        out_shape=[
            jax.ShapeDtypeStruct((8, samples), jnp.float32),
            jax.ShapeDtypeStruct((tables + SUB, hidden_size), jnp.float32),
        ],
        scratch_shapes=[
            pltpu.VMEM((hidden_size, 2 * LANES), jnp.float32),
            pltpu.VMEM((hidden_size, LANES), jnp.float32),
            pltpu.VMEM((hidden_size, LANES), jnp.float32),
        ],
        name="top",
    )(
        gathered,
        received,
        place,
        top_weight.T,
        top_bias.reshape(hidden_size, 1),
        out_weight.astype(jnp.float32).reshape(hidden_size, 1),
        jnp.broadcast_to(out_weight[None, :], (8, hidden_size)),
    )
    if groups == 2:
        grad = grad + lax.ppermute(grad, "grp", [(0, 1), (1, 0)])
    else:
        grad = lax.psum(grad, "grp")
    own = lax.dynamic_slice(logits, (0, lax.axis_index("tab") * LANES), (1, LANES))
    return own.reshape(micro, local_batch), grad[:tables], grad[tables]


def solution(mesh):
    return jax.shard_map(
        per_device,
        mesh=mesh,
        in_specs=(
            P(None, ("grp", "tab"), None),
            P(None, ("grp", "tab"), None),
            P(None, ("grp", "tab"), None),
            P(None, ("grp", "tab")),
            P("tab", None, None),
            P(),
            P(),
            P(),
            P(),
        ),
        out_specs=(P(None, ("grp", "tab")), P(), P()),
        check_vma=False,
    )
```

```python
import functools
import math

import jax
import jax.numpy as jnp
from jax import lax
from jax.experimental import pallas as pl
from jax.experimental.pallas import tpu as pltpu
from jax.sharding import PartitionSpec as P

HOTS = 8
LOSS_SCALE = 32768.0
LANES = 128
SUB = 16
NT = (((1,), (1,)), ((), ()))


def pack_kernel(ids_ref, weights_ref, features_ref, labels_ref, rows_ref, out_ref, *, high, slots):
    members = out_ref.shape[0]
    columns = ids_ref.shape[1]
    block = slots * HOTS
    ids = ids_ref[...].astype(jnp.float32)
    tile = jnp.floor((ids + 0.5) * (1.0 / (SUB * high)))
    rest = ids - tile * (SUB * high)
    hi = jnp.floor((rest + 0.5) * (1.0 / SUB))
    code = rest - hi * SUB + tile * SUB + 128.0
    for bit in (1, 2, 4, 8):
        half = jnp.floor(hi * 0.5)
        code = jnp.where(hi - 2.0 * half > 0.5, code * float(2**bit), code)
        hi = half
    code = code.astype(jnp.bfloat16)
    weights = weights_ref[...]
    eye_r = lax.broadcasted_iota(jnp.int32, (LANES, LANES), 0)
    eye_c = lax.broadcasted_iota(jnp.int32, (LANES, LANES), 1)
    eye = jnp.where(eye_r == eye_c, 1.0, 0.0).astype(jnp.bfloat16)
    turned = lax.dot_general(eye, features_ref[...], NT, preferred_element_type=jnp.float32)
    turned = turned.astype(jnp.bfloat16)
    labels = labels_ref[...].astype(jnp.bfloat16)
    column = lax.broadcasted_iota(jnp.int32, (block, columns), 1)
    for member in range(members):
        rows = rows_ref[member * block : (member + 1) * block, :]
        pick = jnp.where(rows == column, 1.0, 0.0).astype(jnp.bfloat16)
        out_ref[member, 0:block, :] = lax.dot_general(
            pick, code, NT, preferred_element_type=jnp.float32
        ).astype(jnp.bfloat16)
        out_ref[member, block : 2 * block, :] = lax.dot_general(
            pick, weights, NT, preferred_element_type=jnp.float32
        ).astype(jnp.bfloat16)
        out_ref[member, 2 * block : 2 * block + LANES, :] = turned
        out_ref[member, 2 * block + LANES :, :] = labels


def pool_kernel(recv_ref, table_ref, out_ref, hi_ref, lo_ref, w_ref, part_ref, count_ref, acc_ref, *, high, slots, scale):
    slot = pl.program_id(0)
    members = recv_ref.shape[0]
    block = slots * HOTS
    tiles = 128 // SUB

    @pl.when(slot == 0)
    def _():
        def decode(src, carry):
            value = recv_ref[src, 0:block, :].astype(jnp.float32)
            hi = jnp.zeros_like(value)
            for bit in (8, 4, 2, 1):
                big = value >= 128.0 * 2.0**bit
                value = jnp.where(big, value * 2.0**-bit, value)
                hi = jnp.where(big, hi + float(bit), hi)
            hi_ref[src] = hi
            lo_ref[src] = value - 128.0
            w_ref[src] = recv_ref[src, block : 2 * block, :].astype(jnp.float32)
            return carry

        lax.fori_loop(0, members, decode, 0)

    iota = lax.broadcasted_iota(jnp.int32, (SUB, LANES), 0).astype(jnp.float32).astype(jnp.bfloat16)
    zero = jnp.zeros((SUB, LANES), jnp.bfloat16)
    first = pl.multiple_of(slot * HOTS, HOTS)

    def spread(row):
        return jnp.broadcast_to(row, (SUB, LANES)).astype(jnp.bfloat16)

    def pair(index, carry):
        for side in range(2):
            src = index * 2 + side
            hi8 = hi_ref[src, pl.ds(first, HOTS), :]
            lo8 = lo_ref[src, pl.ds(first, HOTS), :]
            w8 = w_ref[src, pl.ds(first, HOTS), :]
            lows = []
            for hot in range(HOTS):
                hi_b = spread(hi8[hot : hot + 1])
                w_b = spread(w8[hot : hot + 1])
                lows.append(spread(lo8[hot : hot + 1]))
                for k in range(high):
                    part_ref[side, hot * high + k] = jnp.where(hi_b == jnp.bfloat16(k), w_b, zero)
            for tile in range(tiles):
                here = iota + jnp.bfloat16(tile * SUB)
                masks = [low == here for low in lows]
                for k in range(high):
                    total = jnp.where(masks[0], part_ref[side, k], zero)
                    for hot in range(1, HOTS):
                        total = total + jnp.where(masks[hot], part_ref[side, hot * high + k], zero)
                    base = (tile * high + k) * SUB
                    count_ref[base : base + SUB, side * LANES : (side + 1) * LANES] = total
        pooled = jnp.dot(table_ref[0], count_ref[...], preferred_element_type=jnp.float32)
        pooled = pooled.astype(jnp.bfloat16).astype(jnp.float32)
        for side in range(2):
            src = index * 2 + side
            turned = recv_ref[src, 2 * block : 2 * block + LANES, :].astype(jnp.float32)
            dots = jnp.sum(pooled[:, side * LANES : (side + 1) * LANES] * turned, axis=0, keepdims=True)
            acc_ref[src, pl.ds(slot, 1), :] = dots * scale
        return carry

    lax.fori_loop(0, members // 2, pair, 0)

    @pl.when(slot == slots - 1)
    def _():
        for src in range(members):
            out_ref[:, src * LANES : (src + 1) * LANES] = acc_ref[src].astype(jnp.bfloat16)


def top_kernel(scores_ref, labels_ref, place_ref, weight_ref, bias_ref, wide_ref, narrow_ref, logits_ref, grad_ref, slope_ref, bias_b, wide_b, *, factor):
    hidden_size = weight_ref.shape[0]
    chunk = 256
    samples = 2 * LANES

    @pl.when(pl.program_id(0) == 0)
    def _():
        grad_ref[...] = jnp.zeros_like(grad_ref)
        bias_b[...] = jnp.broadcast_to(bias_ref[...], bias_b.shape)
        wide_b[...] = jnp.broadcast_to(wide_ref[...], wide_b.shape)

    scores = jnp.dot(place_ref[...], scores_ref[...], preferred_element_type=jnp.float32)
    scores = scores.astype(jnp.bfloat16)
    logits = jnp.zeros((8, samples), jnp.float32)
    for start in range(0, hidden_size, chunk):
        span = slice(start, start + chunk)
        bias = jnp.concatenate([bias_b[span, :]] * 2, axis=1)
        wide = jnp.concatenate([wide_b[span, :]] * 2, axis=1)
        pre = jnp.dot(weight_ref[span, :], scores, preferred_element_type=jnp.float32) + bias
        gate = 0.5 + 0.5 * jnp.tanh(0.5 * pre)
        hidden = pre * gate
        logits = logits + jnp.dot(
            narrow_ref[:, span], hidden.astype(jnp.bfloat16), preferred_element_type=jnp.float32
        )
        slope_ref[span, :] = wide * (gate + hidden * (1.0 - gate))
    logits_ref[...] = logits
    labels = jnp.concatenate([labels_ref[0, 0:1, :], labels_ref[1, 0:1, :]], axis=1)
    delta = (0.5 + 0.5 * jnp.tanh(0.5 * logits[0:1, :]) - labels.astype(jnp.float32)) * factor
    ones = jnp.ones((SUB, samples), jnp.bfloat16)
    left = jnp.concatenate([scores, ones], axis=0)
    for start in range(0, hidden_size, chunk):
        span = slice(start, start + chunk)
        hidden_grad = (slope_ref[span, :] * delta).astype(jnp.bfloat16)
        grad_ref[:, span] += lax.dot_general(left, hidden_grad, NT, preferred_element_type=jnp.float32)


def per_device(
    sample_ids,
    id_weights,
    dense_features,
    click_labels,
    table_shards,
    slot_table,
    top_weight,
    top_bias,
    out_weight,
):
    micro, local_batch, columns = sample_ids.shape
    tables = slot_table.shape[0]
    slots, vocab, width = table_shards.shape
    hidden_size = top_weight.shape[1]
    members = lax.axis_size("tab")
    groups = lax.axis_size("grp")
    local = micro * local_batch
    high = vocab // 128
    assert local == LANES and width == LANES and vocab % 128 == 0 and high <= 16 and members % 2 == 0
    block = slots * HOTS
    height = 2 * block + LANES + SUB
    scale = 1.0 / math.sqrt(width)

    rows = (slot_table[:, None] * HOTS + jnp.arange(HOTS, dtype=jnp.int32)[None, :]).reshape(columns, 1)
    labels = jnp.broadcast_to(click_labels.reshape(1, local), (SUB, local)).astype(jnp.float32)
    packed = pl.pallas_call(
        functools.partial(pack_kernel, high=high, slots=slots),
        out_shape=jax.ShapeDtypeStruct((members, height, LANES), jnp.bfloat16),
        name="pack",
    )(
        sample_ids.reshape(local, columns),
        id_weights.reshape(local, columns),
        dense_features.reshape(local, width),
        labels,
        rows,
    )
    received = lax.all_to_all(packed, "tab", split_axis=0, concat_axis=0, tiled=True)
    turned_tables = jnp.swapaxes(table_shards, 1, 2)
    samples = members * LANES
    scores = pl.pallas_call(
        functools.partial(pool_kernel, high=high, slots=slots, scale=scale),
        grid=(slots,),
        in_specs=[
            pl.BlockSpec((members, height, LANES), lambda s: (0, 0, 0)),
            pl.BlockSpec((1, width, vocab), lambda s: (s, 0, 0)),
        ],
        out_specs=pl.BlockSpec((slots, samples), lambda s: (0, 0)),
        out_shape=jax.ShapeDtypeStruct((slots, samples), jnp.bfloat16),
        scratch_shapes=[
            pltpu.VMEM((members, block, LANES), jnp.float32),
            pltpu.VMEM((members, block, LANES), jnp.float32),
            pltpu.VMEM((members, block, LANES), jnp.float32),
            pltpu.VMEM((2, HOTS * high, SUB, LANES), jnp.bfloat16),
            pltpu.VMEM((vocab, 2 * LANES), jnp.bfloat16),
            pltpu.VMEM((members, slots, LANES), jnp.float32),
        ],
        name="pool",
    )(received, turned_tables)
    copies = jnp.broadcast_to(scores[None], (members, slots, samples))
    gathered = lax.all_to_all(copies, "tab", split_axis=0, concat_axis=0, tiled=True)
    gathered = gathered.reshape(tables, samples)
    place = (jnp.arange(tables, dtype=jnp.int32)[:, None] == slot_table[None, :]).astype(jnp.bfloat16)
    label_block = (2 * block + LANES) // SUB
    logits, grad = pl.pallas_call(
        functools.partial(top_kernel, factor=LOSS_SCALE / (local * members * groups)),
        grid=(members // 2,),
        in_specs=[
            pl.BlockSpec((tables, 2 * LANES), lambda j: (0, j)),
            pl.BlockSpec((2, SUB, LANES), lambda j: (j, label_block, 0)),
            pl.BlockSpec((tables, tables), lambda j: (0, 0)),
            pl.BlockSpec((hidden_size, tables), lambda j: (0, 0)),
            pl.BlockSpec((hidden_size, 1), lambda j: (0, 0)),
            pl.BlockSpec((hidden_size, 1), lambda j: (0, 0)),
            pl.BlockSpec((8, hidden_size), lambda j: (0, 0)),
        ],
        out_specs=[
            pl.BlockSpec((8, 2 * LANES), lambda j: (0, j)),
            pl.BlockSpec((tables + SUB, hidden_size), lambda j: (0, 0)),
        ],
        out_shape=[
            jax.ShapeDtypeStruct((8, samples), jnp.float32),
            jax.ShapeDtypeStruct((tables + SUB, hidden_size), jnp.float32),
        ],
        scratch_shapes=[
            pltpu.VMEM((hidden_size, 2 * LANES), jnp.float32),
            pltpu.VMEM((hidden_size, LANES), jnp.float32),
            pltpu.VMEM((hidden_size, LANES), jnp.float32),
        ],
        name="top",
    )(
        gathered,
        received,
        place,
        top_weight.T,
        top_bias.reshape(hidden_size, 1),
        out_weight.astype(jnp.float32).reshape(hidden_size, 1),
        jnp.broadcast_to(out_weight[None, :], (8, hidden_size)),
    )
    if groups == 2:
        grad = grad + lax.ppermute(grad, "grp", [(0, 1), (1, 0)])
    else:
        grad = lax.psum(grad, "grp")
    own = lax.dynamic_slice(logits, (0, lax.axis_index("tab") * LANES), (1, LANES))
    return own.reshape(micro, local_batch), grad[:tables], grad[tables]


def solution(mesh):
    return jax.shard_map(
        per_device,
        mesh=mesh,
        in_specs=(
            P(None, ("grp", "tab"), None),
            P(None, ("grp", "tab"), None),
            P(None, ("grp", "tab"), None),
            P(None, ("grp", "tab")),
            P("tab", None, None),
            P(),
            P(),
            P(),
            P(),
        ),
        out_specs=(P(None, ("grp", "tab")), P(), P()),
        check_vma=False,
    )
```
